32 devices in a mesh: ta: 4 (over x, core), tb: 8 (over z, y).
Axes of the slice: x: 2, y: 2, z: 4, core: 2. Of those that a mesh axis runs over, the one named last changes fastest.
Arguments:
- theta_cube: bfloat16 [32, 90, 4096], P(('ta', 'tb')), may hold values from -20 to 20, as said below
- station_permutation_map: int32 [128], replicated, may hold values from 0 to 127, each once
- station_bathymetry_group: int32 [4096], replicated, may hold values from 0 to 15
- baroclinic_basis: bfloat16 [16, 90, 90], replicated, may hold values from -0.625 to 0.625
Outputs:
- anomaly_coef: bfloat16 [90, 32, 4096], P(None, None, ('ta', 'tb'))
The draws below stay inside these ranges and needn't reach their ends.
Inputs may be any that keep to these rules, and one draw needn't show every extreme that they name: `theta_cube`: temperature is a level-and-column profile plus time variation.
All inputs are finite; a program needn't handle non-finite values.
Results may differ from the reference program's by a relative error of at most 0.001.
Values may be sent and summed in bfloat16 or wider, within the bound.
No kernel may reach another device: no remote copies, remote signals or barrier semaphores. Data moves between devices by JAX's collectives and lax.ppermute only.
A program may use at most 128 MiB of HBM per device.

```python
import jax
import jax.numpy as jnp
from jax import lax

LEV = 90
MODES = 90
CLASSES = 16
TILE = 32
PROBES_PER_CHIP = 128
SNAPS = 32
COLS = 4096
GROUPS = 128


def draw_theta_cube(key, part):
    first, second = jax.random.split(key, 2)
    profile = jax.random.uniform(first, (1, LEV, COLS), minval=-4.0, maxval=4.0)
    noise = jnp.clip(jax.random.normal(second, (SNAPS, LEV, COLS)), -6.0, 6.0)
    return (profile + noise).astype(jnp.bfloat16)


def set_ends(array, key, low, top_value):
    place = [jax.random.randint(jax.random.fold_in(key, axis), (), 0, length) for axis, length in enumerate(array.shape)]
    widest = array.shape.index(max(array.shape))
    neighbour = place[:widest] + [(place[widest] + 1) % array.shape[widest]] + place[widest + 1:]
    return array.at[tuple(place)].set(low).at[tuple(neighbour)].set(top_value)


def scatter_about(key, extent, spread, bound, kind=jnp.bfloat16):
    values = spread * jax.random.normal(key, extent, jnp.float32)
    return jnp.clip(values, min=-bound, max=bound).astype(kind)


def setup_inputs(seed: int = 0) -> dict:
    arg_keys = jax.random.split(jax.random.key(seed), 5)
    return {
        "theta_cube": draw_theta_cube(jax.random.fold_in(arg_keys[4], 71), 0),
        "station_permutation_map": jax.random.permutation(arg_keys[1], GROUPS).astype(jnp.int32),
        "station_bathymetry_group": set_ends(jax.random.randint(arg_keys[2], (COLS,), 0, CLASSES), jax.random.fold_in(arg_keys[2], 1), 0, CLASSES - 1).astype(jnp.int32),
        "baroclinic_basis": scatter_about(arg_keys[3], (CLASSES, LEV, MODES), LEV ** -0.5, 0.625),
    }


def reference(theta_cube, station_permutation_map, station_bathymetry_group, baroclinic_basis):
    offsets = jnp.arange(TILE, dtype=jnp.int32)
    source = (station_permutation_map.astype(jnp.int32)[:, None] * TILE + offsets[None, :]).reshape(-1)

    def one_block(probe_ordinal):
        probe_thermal_readings = jnp.take(theta_cube, probe_ordinal, axis=2).astype(jnp.float32)
        selected_probes = jnp.take(baroclinic_basis, jnp.take(station_bathymetry_group, probe_ordinal, axis=0), axis=0).astype(jnp.float32)
        modal_amplitude = jnp.einsum('btq,qtf->fbq', probe_thermal_readings, selected_probes)
        mean_coef = jnp.mean(modal_amplitude, axis=1, keepdims=True)
        return (modal_amplitude - mean_coef).astype(jnp.bfloat16)

    blocks = lax.map(one_block, source.reshape(-1, PROBES_PER_CHIP).astype(jnp.int32))
    return jnp.transpose(blocks, (1, 2, 0, 3)).reshape(MODES, SNAPS, COLS)
```

```python
import jax
import jax.numpy as jnp
from jax import lax
from jax.experimental import pallas as pl
from jax.experimental.pallas import tpu as pltpu
from jax.sharding import PartitionSpec as P

TILE = 32
LANES = 128
PACK = 16


def round_up(value, step):
    return -(-value // step) * step


def column_block(read, perm_ref, first_group, lane_group, tiles):
    block = None
    for slot in range(tiles):
        group = perm_ref[first_group + slot]
        piece = read(group // tiles)
        piece = pltpu.roll(piece, lax.rem(slot + tiles - lax.rem(group, tiles), tiles) * TILE, 1)
        block = piece if block is None else jnp.where(lane_group == slot, piece, block)
    return block


def regroup_kernel(perm_ref, theta_ref, out_ref):
    dests, levels_pad, width = out_ref.shape
    levels = theta_ref.shape[0]
    tiles = width // TILE
    lane_group = lax.broadcasted_iota(jnp.int32, (levels, width), 1) // TILE

    def read(index):
        return theta_ref[:, pl.ds(pl.multiple_of(index * width, width), width)].astype(jnp.float32)

    def one(dest, carry):
        block = column_block(read, perm_ref, dest * tiles, lane_group, tiles)
        out_ref[dest, 0:levels, :] = block.astype(out_ref.dtype)
        out_ref[dest, levels:levels_pad, :] = jnp.zeros((levels_pad - levels, width), out_ref.dtype)
        return carry

    lax.fori_loop(0, dests, one, 0)


def modes_kernel(perm_ref, owner_ref, classes_ref, basis_ref, recv_ref, out_ref, weight_ref, coef_ref):
    snaps, levels_pad, width = recv_ref.shape
    classes, levels, modes = basis_ref.shape
    tiles = width // TILE
    modes_pad = weight_ref.shape[0]
    lane_group = lax.broadcasted_iota(jnp.int32, (8, width), 1) // TILE

    def read(index):
        return jnp.broadcast_to(classes_ref[pl.ds(index, 1), :], (8, width))

    mine = column_block(read, perm_ref, owner_ref[0] * tiles, lane_group, tiles)
    mine = jnp.broadcast_to(mine[0:1].astype(jnp.float32), (levels_pad, width)).astype(jnp.bfloat16)

    for c in range(classes):
        square = jnp.pad(basis_ref[c].astype(jnp.float32), ((0, LANES - levels), (0, LANES - modes)))
        square = square.T[0:modes_pad, 0:levels_pad]
        weight_ref[:, c * levels_pad:(c + 1) * levels_pad] = square.astype(jnp.bfloat16)

    group = 2

    def one(step, total):
        cols = []
        for t in range(group):
            value = recv_ref[step * group + t]
            cols.append(jnp.concatenate(
                [jnp.where(mine == jnp.bfloat16(c), value, jnp.bfloat16(0)) for c in range(classes)], axis=0))
        both = jnp.concatenate(cols, axis=1)
        coef = jnp.dot(weight_ref[...], both, preferred_element_type=jnp.float32)
        for t in range(group):
            piece = coef[0:modes, t * width:(t + 1) * width]
            total = total + piece
            coef_ref[pl.ds(step * group + t, modes, stride=snaps), :] = piece
        return total

    total = lax.fori_loop(0, snaps // group, one, jnp.zeros((modes, width), jnp.float32))
    mean = total * (1.0 / snaps)
    for m in range(modes):
        rows = coef_ref[m * snaps:(m + 1) * snaps, :]
        out_ref[m] = (rows - mean[m:m + 1]).astype(out_ref.dtype)


def on_device(theta_cube, station_permutation_map, station_bathymetry_group, baroclinic_basis):
    instants, levels, columns = theta_cube.shape
    classes, _, modes = baroclinic_basis.shape
    devices = lax.axis_size("ta") * lax.axis_size("tb")
    width = columns // devices
    snaps = devices * instants
    levels_pad = round_up(levels, PACK)
    modes_pad = round_up(modes, PACK)
    owner = (lax.axis_index("ta") * lax.axis_size("tb") + lax.axis_index("tb")).astype(jnp.int32)
    smem = pl.BlockSpec(memory_space=pltpu.SMEM)
    vmem = pl.BlockSpec(memory_space=pltpu.VMEM)
    regrouped = pl.pallas_call(
        regroup_kernel,
        out_shape=jax.ShapeDtypeStruct((devices, levels_pad, width), theta_cube.dtype),
        in_specs=[smem, vmem],
        out_specs=vmem,
    )(station_permutation_map, theta_cube.reshape(levels, columns))
    moved = lax.all_to_all(regrouped, ("ta", "tb"), split_axis=0, concat_axis=0, tiled=True)
    return pl.pallas_call(
        modes_kernel,
        out_shape=jax.ShapeDtypeStruct((modes, snaps, width), jnp.bfloat16),
        in_specs=[smem, smem, vmem, vmem, vmem],
        out_specs=vmem,
        scratch_shapes=[
            pltpu.VMEM((modes_pad, classes * levels_pad), jnp.bfloat16),
            pltpu.VMEM((modes * snaps, width), jnp.float32),
        ],
    )(station_permutation_map, owner.reshape(1), station_bathymetry_group.reshape(-1, width), baroclinic_basis, moved)


def solution(mesh):
    return jax.shard_map(
        on_device,
        mesh=mesh,
        in_specs=(P(("ta", "tb"), None, None), P(), P(), P()),
        out_specs=P(None, None, ("ta", "tb")),
        check_vma=False,
    )
```
